128 devices in a mesh: fsdp: 32 (over y, z_lo, x), tp: 4 (over z_hi, core).
Axes of the slice: x: 4, y: 4, z: 4 (z_hi: 2, z_lo: 2; z = z_hi * 2 + z_lo), core: 2. Of those that a mesh axis runs over, the one named last changes fastest.
Arguments:
- partials: bfloat16 [32, 2, 5120, 1024], P('fsdp', None, None, 'tp'), may hold values from -6 to 6
- token_counts: int32 [32], P('fsdp'), may hold values from 100 to 599
- owner_map: int32 [2, 4], replicated, may hold values from 0 to 3, each once within a row
- params: float32 [2, 5120, 1024], P(None, 'fsdp', 'tp'), may hold values from -0.75 to 0.75
- moment1: float32 [2, 5120, 1024], P(None, 'fsdp', 'tp'), may hold values from -0.15625 to 0.15625
- moment2: float32 [2, 5120, 1024], P(None, 'fsdp', 'tp'), may hold values from 0.0001 to 0.004
Outputs:
- new_params: float32 [2, 5120, 1024], P(None, 'fsdp', 'tp')
- new_moment1: float32 [2, 5120, 1024], P(None, 'fsdp', 'tp')
- new_moment2: float32 [2, 5120, 1024], P(None, 'fsdp', 'tp')
- rollout_delta: bfloat16 [2, 5120, 1024], P(None, None, 'tp')
The draws below stay inside these ranges and needn't reach their ends.
Inputs may be any that keep to these rules, and one draw needn't show every extreme that they name: `owner_map`: each row is a permutation of 0 to 3.
All inputs are finite; a program needn't handle non-finite values.
Results may differ from the reference program's by a relative error of at most 0.0004.
Values may be sent and summed in bfloat16 or wider, within the bound.
A program may use at most 64 MiB of HBM per device.

```python
import math
import jax
import jax.numpy as jnp
from jax import lax

D = 5120
KV = 1024
LAYERS = 2
STEP = 10
N_FSDP = 32
N_TP = 4


def draw_token_counts(key, part):
    base = jax.random.randint(key, (N_FSDP,), 100, 200)
    ramp = jnp.arange(N_FSDP, dtype=jnp.int32) * 400 // max(N_FSDP - 1, 1)
    position = jnp.arange(N_FSDP, dtype=jnp.int32)
    counts = jnp.where(position == 0, 100, base + ramp)
    counts = jnp.where(position == N_FSDP - 1, 599, counts)
    return counts.astype(jnp.int32)


def spiked(values, own_key, source, target, shards_of, factor):
    def block_of(dim):
        return (jnp.arange(values.shape[dim]) // (values.shape[dim] // shards_of)).reshape((-1,) + (1,) * (values.ndim - 1 - dim))

    near = jax.random.permutation(own_key, shards_of)[block_of(target)]
    far = (block_of(target) + shards_of // 2) % shards_of
    return jnp.where((block_of(source) == near) | (block_of(source) == far), factor * values, values)


def block_levels(key, shape, cuts, least, largest):
    loudness = 1.0
    for dim, blocks in cuts:
        draws = jax.random.uniform(jax.random.fold_in(jax.random.fold_in(key, 6), dim), (blocks,), jnp.float32, least / len(cuts), largest / len(cuts))
        loudness = loudness * jnp.repeat(jnp.exp(draws), shape[dim] // blocks).reshape((-1,) + (1,) * (len(shape) - 1 - dim))
    return loudness


def scatter_about(stream_key, dims, width, limit, pieces=(), held_as=jnp.bfloat16):
    drawn = jax.random.normal(stream_key, dims, jnp.float32) * width
    if len(pieces) > 0:
        drawn = block_levels(stream_key, dims, pieces, -0.22, 0.18) * drawn
    return jnp.clip(drawn, min=-limit, max=limit).astype(held_as)


def bell_draw_with(rng, extent, scale, reach, split, heavy, kind=jnp.bfloat16):
    drawn = scale * jax.random.normal(rng, extent, jnp.float32)
    if split:
        drawn = drawn * block_levels(rng, extent, split, -0.22, 0.18)
    return jnp.clip(spiked(drawn, jax.random.fold_in(rng, 3), *heavy), -reach, reach).astype(kind)


def setup_inputs(seed: int = 0) -> dict:
    streams_of = jax.random.split(jax.random.key(seed), 7)
    return {
        "partials": bell_draw_with(streams_of[0], (N_FSDP, LAYERS, D, KV), 1.0, 6.0, ((0, 32), (3, 4)), (0, 2, 32, 2.75)),
        "token_counts": draw_token_counts(jax.random.fold_in(streams_of[6], 71), 0),
        "owner_map": jax.vmap(lambda own: jax.random.permutation(own, N_TP))(jax.random.split(streams_of[2], LAYERS)).reshape((LAYERS, N_TP)).astype(jnp.int32),
        "params": scatter_about(streams_of[3], (LAYERS, D, KV), 0.05, 0.75, ((1, 32), (2, 4)), jnp.float32),
        "moment1": scatter_about(streams_of[4], (LAYERS, D, KV), 0.01, 0.15625, ((1, 32), (2, 4)), jnp.float32),
        "moment2": jnp.clip(jnp.exp(math.log(0.004) - 3.6888795 * jax.random.uniform(streams_of[5], (LAYERS, D, KV), jnp.float32) ** block_levels(streams_of[5], (LAYERS, D, KV), ((1, 32), (2, 4)), -0.2, 0.2)), 0.0001, 0.004),
    }


def reference(partials, token_counts, owner_map, params, moment1, moment2):
    weights = token_counts.astype(jnp.float32)
    total = jnp.sum(weights)

    def accumulate(summed, pair):
        term, weight = pair
        return (summed + weight * term.astype(jnp.float32), None)
    summed, _ = lax.scan(accumulate, jnp.zeros((LAYERS, D, KV), jnp.float32), (partials, weights))
    grad = summed / total
    first = 0.9 * moment1 + 0.1 * grad
    second = 0.999 * moment2 + 0.001 * grad * grad
    bias_one = 1.0 - 0.9 ** STEP
    bias_two = 1.0 - 0.999 ** STEP
    direction = first / bias_one / (jnp.sqrt(second / bias_two) + 1e-08)
    new_params = params - 0.001 * (direction + 0.1 * params)
    delta = direction.astype(jnp.bfloat16)
    blocks = delta.reshape(LAYERS, D, N_TP, KV // N_TP)
    chosen = owner_map.astype(jnp.int32)[:, None, :, None]
    rollout = jnp.take_along_axis(blocks, chosen, axis=2).reshape(LAYERS, D, KV)
    return (new_params, first, second, rollout)
```

```python
import functools

import jax
import jax.numpy as jnp
from jax import lax
from jax.experimental import pallas as pl
from jax.experimental.pallas import tpu as pltpu
from jax.sharding import Mesh
from jax.sharding import PartitionSpec as P

STEP = 10
AXES = ("y", "zl", "x", "zh", "core")
FSDP = ("y", "zl", "x")
TP = ("zh", "core")
MESH = pl.DeviceIdType.MESH
F32 = jnp.float32
BF16 = jnp.bfloat16
GROUP = 32
ORDER = (2, 1, 3, 0)


def kernel(
    part, count, owners, par, mom1, mom2,
    new_par, new_mom1, new_mom2, out,
    own, got1, sent2, total, got2, got3, weight, weight1, weight2, weight3, cand0, cand1, par_v, mom1_v, mom2_v,
    local_sem, own_sem, s1, q1, s2, q2, s3, q3, ws, wq, ts, tq, as_, aq, zs, zq, cs, cq, hs, hq,
):
    at = {name: lax.axis_index(name) for name in AXES}
    z = at["zl"]
    me_tp = at["zh"] * 2 + at["core"]
    rows = got3.shape[2]
    cols = got3.shape[3]
    half = rows // 2
    first_axis = ("x", "y")
    last_axis = ("y", "x")
    pending = []
    cands = (cand0, cand1)

    def shifted(name, by, size):
        return lax.rem(at[name] + by, size)

    def send(src, dst, ssem, rsem, device):
        copy = pltpu.make_async_remote_copy(
            src_ref=src, dst_ref=dst, send_sem=ssem, recv_sem=rsem, device_id=device, device_id_type=MESH
        )
        copy.start()
        pending.append(copy)

    def arrived(dst, ssem, rsem, device):
        pltpu.make_async_remote_copy(
            src_ref=dst, dst_ref=dst, send_sem=ssem, recv_sem=rsem, device_id=device, device_id_type=MESH
        ).wait_recv()

    other_z = {"zl": 1 - z}
    other_zh = {"zh": 1 - at["zh"]}
    other_core = {"core": 1 - at["core"]}

    state = [
        pltpu.make_async_copy(par, par_v, local_sem.at[0]),
        pltpu.make_async_copy(mom1, mom1_v, local_sem.at[1]),
        pltpu.make_async_copy(mom2, mom2_v, local_sem.at[2]),
    ]
    own_copies = {}

    def block_of(l, k, to):
        c = shifted(last_axis[l], k, 4)
        a = shifted(first_axis[l], to, 4)
        return part.at[0, c, :, a] if l == 0 else part.at[1, a, :, c]

    weight[0] = jnp.full(weight.shape[1:], count[0].astype(F32), F32)
    for l in range(2):
        for k in ORDER:
            copy = pltpu.make_async_copy(block_of(l, k, 0), own.at[l, k], own_sem.at[l, k])
            copy.start()
            own_copies[l, k] = copy
    for copy in state:
        copy.start()

    barrier = pltpu.get_barrier_semaphore()
    peers = [{n: shifted(n, d, 4)} for n in ("x", "y") for d in (1, 2, 3)] + [other_z, other_zh, other_core]
    for peer in peers:
        pl.semaphore_signal(barrier, inc=1, device_id=peer, device_id_type=MESH)
    pl.semaphore_wait(barrier, len(peers))

    def to_first(l, d):
        return {first_axis[l]: shifted(first_axis[l], d, 4)}

    def to_last(l, d):
        return {last_axis[l]: shifted(last_axis[l], d, 4)}

    for k in ORDER:
        for l in range(2):
            for d in (2, 1, 3):
                send(block_of(l, k, d), got1.at[l, d - 1, k], s1.at[l, d - 1, k], q1.at[l, d - 1, k], to_first(l, d))
        if k == ORDER[0]:
            for l in range(2):
                for d in (1, 2, 3):
                    i = l * 3 + d - 1
                    send(weight.at[0], weight1.at[i], ws.at[i], wq.at[i], to_first(l, d))

    def row_loop(body):
        def step(i, carry):
            body(pl.ds(pl.multiple_of(i * GROUP, GROUP), GROUP))
            return carry

        lax.fori_loop(0, rows // GROUP, step, 0)

    def sum_first(l, k, which, dst):
        w = [weight[0, 0:1, :]] + [weight1[l * 3 + d, 0:1, :] for d in range(3)]

        def body(r):
            t = own[l, k, which, r, :].astype(F32) * w[0]
            for d in range(3):
                t = t + got1[l, d, k, which, r, :].astype(F32) * w[d + 1]
            dst[l, k, r, :] = t

        row_loop(body)

    def stage1(l, k):
        own_copies[l, k].wait()
        for d in range(3):
            arrived(got1.at[l, d, k], s1.at[l, d, k], q1.at[l, d, k], to_first(l, d + 1))
        sum_first(l, k, 1 - z, sent2)
        sum_first(l, k, z, total)
        send(sent2.at[l, k], got2.at[l, k], s2.at[l, k], q2.at[l, k], other_z)

    def stage2(l, k):
        arrived(got2.at[l, k], s2.at[l, k], q2.at[l, k], other_z)

        def body(r):
            total[l, k, r, :] = total[l, k, r, :] + got2[l, k, r, :]

        row_loop(body)
        if k:
            send(total.at[l, k], got3.at[l, k - 1], s3.at[l, k - 1], q3.at[l, k - 1], to_last(l, k))

    for i in range(6):
        arrived(weight1.at[i], ws.at[i], wq.at[i], to_first(i // 3, i % 3 + 1))
    weight[1] = weight[0] + weight1[0] + weight1[1] + weight1[2]

    units = [(l, k) for k in ORDER for l in range(2)]
    for n, (l, k) in enumerate(units):
        stage1(l, k)
        if n == 0:
            send(weight.at[1], weight2, ws.at[6], wq.at[6], other_z)
        if n >= 2:
            if n == 2:
                arrived(weight2, ws.at[6], wq.at[6], other_z)
                weight[2] = weight[1] + weight2[...]
            stage2(*units[n - 2])
            if n == 2:
                for d in (1, 2, 3):
                    send(weight.at[2], weight3.at[d - 1], ws.at[6 + d], wq.at[6 + d], to_last(0, d))
    stage2(*units[-2])
    stage2(*units[-1])

    for copy in state:
        copy.wait()
    for d in range(3):
        arrived(weight3.at[d], ws.at[7 + d], wq.at[7 + d], to_last(0, d + 1))
    inverse = 1.0 / (weight[2] + weight3[0] + weight3[1] + weight3[2])
    scale = inverse[0:1, :]
    inv_one = 1.0 / (1.0 - 0.9**STEP)
    inv_two = 1.0 / (1.0 - 0.999**STEP)

    def update(l):
        for d in (1, 0, 2):
            arrived(got3.at[l, d], s3.at[l, d], q3.at[l, d], to_last(l, d + 1))

        def body(r):
            grad = (total[l, 0, r, :] + got3[l, 0, r, :] + got3[l, 1, r, :] + got3[l, 2, r, :]) * scale
            first = 0.9 * mom1_v[l, r, :] + 0.1 * grad
            second = 0.999 * mom2_v[l, r, :] + 0.001 * grad * grad
            direction = (first * inv_one) / (jnp.sqrt(second * inv_two) + 1e-08)
            old = par_v[l, r, :]
            new_par[l, r, :] = old - 0.001 * (direction + 0.1 * old)
            new_mom1[l, r, :] = first
            new_mom2[l, r, :] = second
            cands[l][me_tp, r, :] = direction.astype(BF16)

        row_loop(body)

    tp_zh = (1 - at["zh"]) * 2 + at["core"]
    tp_core = at["zh"] * 2 + 1 - at["core"]
    tp_both = (1 - at["zh"]) * 2 + 1 - at["core"]
    for l in range(2):
        update(l)
        mine = cands[l].at[me_tp]
        send(mine, mine, ts.at[l, 0], tq.at[l, 0], other_zh)
        send(mine, mine, ts.at[l, 1], tq.at[l, 1], other_core)

    def place(l, fl, zz, ll):
        return out.at[l, ll, zz, fl] if l == 0 else out.at[l, fl, zz, ll]

    def block(l, ka, oz, kc):
        a = shifted(first_axis[l], 4 - ka, 4)
        c = shifted(last_axis[l], 4 - kc, 4)
        return place(l, a, 1 - z if oz else z, c)

    def spread_last(l, p):
        b = block(l, p % 4, p // 4, 0)
        send(b, b, cs.at[l, 0, p], cq.at[l, 0, p], to_last(l, 1))
        send(b, b, cs.at[l, 1, p], cq.at[l, 1, p], to_last(l, 3))

    def spread_z(l, d):
        b = block(l, d, 0, 0)
        send(b, b, zs.at[l, d], zq.at[l, d], other_z)

    for l in range(2):
        theirs = cands[l].at[tp_zh]
        arrived(theirs, ts.at[l, 0], tq.at[l, 0], other_zh)
        send(theirs, theirs, ts.at[l, 2], tq.at[l, 2], other_core)
    for l in range(2):
        arrived(cands[l].at[tp_core], ts.at[l, 1], tq.at[l, 1], other_core)
        arrived(cands[l].at[tp_both], ts.at[l, 2], tq.at[l, 2], other_core)
        wanted = owners[l, me_tp]
        mine = block(l, 0, 0, 0)

        def body(r):
            mine[r, :] = cands[l][wanted, r, :]

        row_loop(body)
        for d in (1, 3, 2):
            send(mine, mine, as_.at[l, d - 1], aq.at[l, d - 1], to_first(l, d))
        spread_z(l, 0)
        spread_last(l, 0)

    def from_first(l, d):
        arrived(block(l, d, 0, 0), as_.at[l, d - 1], aq.at[l, d - 1], to_first(l, d))
        spread_z(l, d)
        spread_last(l, d)

    def from_z(l, d):
        arrived(block(l, d, 1, 0), zs.at[l, d], zq.at[l, d], other_z)
        spread_last(l, 4 + d)

    def relay(l, p):
        for way, (kc, to) in enumerate(((1, 1), (3, 3))):
            b = block(l, p % 4, p // 4, kc)
            arrived(b, cs.at[l, way, p], cq.at[l, way, p], to_last(l, to))
            piece = b.at[pl.ds(way * half, half)]
            send(piece, piece, hs.at[l, way, p], hq.at[l, way, p], to_last(l, to))

    steps = [
        (from_first, 1), (from_first, 3), (relay, 0), (from_z, 0), (from_first, 2), (relay, 1), (relay, 3), (relay, 4),
        (from_z, 1), (from_z, 3), (from_z, 2), (relay, 2), (relay, 5), (relay, 7), (relay, 6),
    ]
    for step, i in steps:
        for l in range(2):
            step(l, i)
    for _, i in [s for s in steps if s[0] is relay]:
        for l in range(2):
            for way in range(2):
                b = block(l, i % 4, i // 4, 2).at[pl.ds(way * half, half)]
                arrived(b, hs.at[l, way, i], hq.at[l, way, i], to_last(l, 1 + 2 * way))
    for copy in pending:
        copy.wait_send()


def local(partials, token_counts, owner_map, params, moment1, moment2):
    layers, shard, cols = params.shape
    blocks = partials.reshape(layers, 4, 2, 4, shard, cols)
    hbm = pl.BlockSpec(memory_space=pltpu.HBM)
    smem = pl.BlockSpec(memory_space=pltpu.SMEM)
    vmem = pl.BlockSpec(memory_space=pltpu.VMEM)
    dma = pltpu.SemaphoreType.DMA
    tile = (shard, cols)
    new_params, first, second, rollout = pl.pallas_call(
        kernel,
        out_shape=(
            pltpu.VMEM(params.shape, F32),
            pltpu.VMEM(params.shape, F32),
            pltpu.VMEM(params.shape, F32),
            pltpu.VMEM((layers, 4, 2, 4, *tile), BF16),
        ),
        in_specs=[hbm, smem, smem, hbm, hbm, hbm],
        out_specs=(vmem, vmem, vmem, vmem),
        scratch_shapes=[
            pltpu.VMEM((2, 4, 2, *tile), BF16),
            pltpu.VMEM((2, 3, 4, 2, *tile), BF16),
            pltpu.VMEM((2, 4, *tile), F32),
            pltpu.VMEM((2, 4, *tile), F32),
            pltpu.VMEM((2, 4, *tile), F32),
            pltpu.VMEM((2, 3, *tile), F32),
            pltpu.VMEM((3, 8, cols), F32),
            pltpu.VMEM((6, 8, cols), F32),
            pltpu.VMEM((8, cols), F32),
            pltpu.VMEM((3, 8, cols), F32),
            pltpu.VMEM((4, *tile), BF16),
            pltpu.VMEM((4, *tile), BF16),
            pltpu.VMEM(params.shape, F32),
            pltpu.VMEM(params.shape, F32),
            pltpu.VMEM(params.shape, F32),
            dma((3,)),
            dma((2, 4)),
            dma((2, 3, 4)), dma((2, 3, 4)),
            dma((2, 4)), dma((2, 4)),
            dma((2, 3)), dma((2, 3)),
            dma((10,)), dma((10,)),
            dma((2, 3)), dma((2, 3)),
            dma((2, 3)), dma((2, 3)),
            dma((2, 4)), dma((2, 4)),
            dma((2, 2, 8)), dma((2, 2, 8)),
            dma((2, 2, 8)), dma((2, 2, 8)),
        ],
        compiler_params=pltpu.CompilerParams(
            collective_id=0, has_side_effects=True, vmem_limit_bytes=56 * 2**20
        ),
        name="reduce_update_spread",
    )(blocks, token_counts, owner_map, params, moment1, moment2)
    return new_params, first, second, rollout.reshape(layers, 32 * shard, cols)


def solution(mesh):
    split = Mesh(mesh.devices.reshape(4, 2, 4, 2, 2), AXES)
    return jax.shard_map(
        local,
        mesh=split,
        in_specs=(
            P(FSDP, None, None, TP),
            P(FSDP),
            P(),
            P(None, FSDP, TP),
            P(None, FSDP, TP),
            P(None, FSDP, TP),
        ),
        out_specs=(P(None, FSDP, TP), P(None, FSDP, TP), P(None, FSDP, TP), P(None, None, TP)),
        check_vma=False,
    )
```

```python
import jax
import jax.numpy as jnp
from jax import lax
from jax.experimental import pallas as pl
from jax.experimental.pallas import tpu as pltpu
from jax.sharding import Mesh
from jax.sharding import PartitionSpec as P

STEP = 10
AXES = ("y", "zl", "x", "zh", "core")
FSDP = ("y", "zl", "x")
TP = ("zh", "core")
MESH = pl.DeviceIdType.MESH
F32 = jnp.float32
BF16 = jnp.bfloat16
GROUP = 32
ORDER = (2, 1, 3, 0)
SPLITS = (96, 64)
STARTS = tuple(sum(SPLITS[:i]) for i in range(len(SPLITS)))
AHEAD = 2
EVENTS = [
    ("s1", 0, 0, 2), ("s1", 0, 1, 2), ("s1", 0, 0, 1), ("s1", 0, 1, 1), ("s2", 0, 0, 2), ("s2", 0, 1, 2),
    ("s1", 0, 0, 3), ("s1", 0, 1, 3), ("s2", 0, 0, 1), ("s2", 0, 1, 1), ("s1", 0, 0, 0), ("s1", 0, 1, 0),
    ("s2", 0, 0, 3), ("m", 0, 0, 1), ("m", 0, 0, 3), ("m", 0, 1, 1), ("m", 0, 1, 3), ("s2", 0, 1, 3),
    ("s1", 1, 0, 2), ("s1", 1, 1, 2), ("s2", 0, 0, 0), ("s1", 1, 0, 1), ("s1", 1, 1, 1), ("s2", 0, 1, 0),
    ("s2", 1, 0, 2), ("fin", 0, 0), ("fin", 0, 1), ("s2", 1, 1, 2), ("s2", 1, 0, 1), ("s1", 1, 0, 3),
    ("s1", 1, 1, 3), ("s2", 1, 1, 1), ("tz", 0, 0), ("tz", 0, 1), ("ag", 0, 0), ("s1", 1, 0, 0), ("s1", 1, 1, 0),
    ("ag", 0, 1), ("m", 1, 0, 1), ("m", 1, 0, 3), ("m", 1, 1, 1), ("m", 1, 1, 3), ("s2", 1, 0, 3), ("s2", 1, 1, 3),
    ("A", 0, 0, 1), ("A", 0, 0, 3), ("C", 0, 0, 0, 1), ("C", 0, 0, 0, 3), ("Z", 0, 0, 0), ("A", 0, 1, 1),
    ("A", 0, 1, 3), ("A", 0, 0, 2), ("C", 0, 1, 0, 1), ("C", 0, 1, 0, 3), ("s2", 1, 0, 0), ("A", 0, 1, 2),
    ("s2", 1, 1, 0), ("fin", 1, 1), ("fin", 1, 0), ("C", 0, 1, 1, 1), ("C", 0, 1, 1, 3), ("Z", 0, 1, 0),
    ("C", 0, 0, 1, 1), ("C", 0, 0, 1, 3), ("C", 0, 1, 3, 1), ("C", 0, 1, 3, 3), ("Z", 0, 0, 1), ("C", 0, 0, 3, 1),
    ("C", 0, 0, 3, 3), ("Z", 0, 0, 3), ("C", 0, 1, 2, 1), ("C", 0, 1, 2, 3), ("tz", 1, 1), ("C", 0, 0, 4, 1),
    ("C", 0, 0, 4, 3), ("Z", 0, 1, 1), ("tz", 1, 0), ("ag", 1, 1), ("C", 0, 0, 2, 1), ("C", 0, 0, 2, 3),
    ("C", 0, 1, 4, 1), ("C", 0, 1, 4, 3), ("Z", 0, 1, 3), ("ag", 1, 0), ("Z", 0, 0, 2), ("C", 0, 0, 5, 1),
    ("C", 0, 0, 5, 3), ("C", 0, 1, 5, 1), ("C", 0, 1, 5, 3), ("Z", 0, 1, 2), ("C", 0, 0, 7, 1), ("C", 0, 0, 7, 3),
    ("C", 1, 1, 0, 1), ("C", 1, 1, 0, 3), ("Z", 1, 1, 0), ("A", 1, 1, 1), ("A", 1, 1, 3), ("Z", 1, 0, 0),
    ("C", 0, 1, 7, 1), ("C", 0, 1, 7, 3), ("A", 1, 0, 1), ("A", 1, 0, 3), ("A", 1, 1, 2), ("C", 1, 0, 0, 1),
    ("C", 1, 0, 0, 3), ("A", 1, 0, 2), ("Z", 1, 1, 1), ("C", 0, 0, 6, 1), ("C", 0, 0, 6, 3), ("Z", 1, 1, 3),
    ("C", 0, 1, 6, 1), ("C", 0, 1, 6, 3), ("Z", 1, 0, 1), ("C", 1, 1, 4, 1), ("C", 1, 1, 4, 3), ("Z", 1, 0, 3),
    ("C", 1, 0, 4, 1), ("C", 1, 0, 4, 3), ("C", 1, 1, 1, 1), ("C", 1, 1, 1, 3), ("Z", 1, 1, 2), ("C", 1, 0, 1, 1),
    ("C", 1, 0, 1, 3), ("C", 1, 1, 3, 1), ("C", 1, 1, 3, 3), ("Z", 1, 0, 2), ("C", 1, 0, 3, 1), ("C", 1, 0, 3, 3),
    ("C", 1, 1, 2, 1), ("C", 1, 1, 2, 3), ("C", 1, 0, 2, 1), ("C", 1, 0, 2, 3), ("C", 1, 1, 5, 1),
    ("C", 1, 1, 5, 3), ("C", 1, 0, 5, 1), ("C", 1, 0, 5, 3), ("C", 1, 1, 7, 1), ("C", 1, 1, 7, 3),
    ("C", 1, 0, 7, 1), ("C", 1, 0, 7, 3), ("C", 1, 1, 6, 1), ("C", 1, 1, 6, 3), ("C", 1, 0, 6, 1),
    ("C", 1, 0, 6, 3),
]


def kernel(
    part, count_h, owners_h, par, mom1, mom2,
    new_par, new_mom1, new_mom2, out,
    count, owners, own, got1, sent2, total, got2, gotm, got3,
    weight, weight1, weight2, weight3, par_v, mom1_v, mom2_v,
    local_sem, own_sem, s1, q1, s2, q2, sm, qm, s3, q3, ws, wq, ts, tq, as_, aq, zs, zq, cs, cq, hs, hq,
    *cands,
):
    at = {name: lax.axis_index(name) for name in AXES}
    z = at["zl"]
    me_tp = at["zh"] * 2 + at["core"]
    first_axis = ("x", "y")
    last_axis = ("y", "x")
    pending = []
    ready = set()

    def rows_of(h):
        return pl.ds(STARTS[h], SPLITS[h])

    def half_of(h, way):
        n = SPLITS[h] // 2
        return pl.ds(STARTS[h] + (n if way == 3 else 0), n)

    def shifted(name, by, size):
        return lax.rem(at[name] + by, size)

    def to_first(l, d):
        return {first_axis[l]: shifted(first_axis[l], d, 4)}

    def to_last(l, d):
        return {last_axis[l]: shifted(last_axis[l], d, 4)}

    other_z = {"zl": 1 - z}
    other_zh = {"zh": 1 - at["zh"]}
    other_core = {"core": 1 - at["core"]}

    def remote(src, dst, sems, i, device):
        return pltpu.make_async_remote_copy(
            src_ref=src, dst_ref=dst, send_sem=sems[0].at[i], recv_sem=sems[1].at[i], device_id=device, device_id_type=MESH
        )

    def send(*args):
        copy = remote(*args)
        copy.start()
        pending.append(copy)

    def arrived(dst, sems, i, device):
        remote(dst, dst, sems, i, device).wait_recv()

    def block_of(h, l, k, to):
        c = shifted(last_axis[l], k, 4)
        a = shifted(first_axis[l], to, 4)
        return part.at[0, c, :, a, rows_of(h)] if l == 0 else part.at[1, a, :, c, rows_of(h)]

    scalars = [
        pltpu.make_async_copy(count_h, count, local_sem.at[3]),
        pltpu.make_async_copy(owners_h, owners, local_sem.at[4]),
    ]
    state = [
        pltpu.make_async_copy(par, par_v, local_sem.at[0]),
        pltpu.make_async_copy(mom1, mom1_v, local_sem.at[1]),
        pltpu.make_async_copy(mom2, mom2_v, local_sem.at[2]),
    ]
    own_copies = {}
    for copy in scalars:
        copy.start()
    for h in range(len(SPLITS)):
        for k in ORDER:
            for l in range(2):
                copy = pltpu.make_async_copy(block_of(h, l, k, 0), own.at[l, k, :, rows_of(h)], own_sem.at[h, l, k])
                copy.start()
                own_copies[h, l, k] = copy
    for copy in state:
        copy.start()
    for copy in scalars:
        copy.wait()
    weight[0] = jnp.full(weight.shape[1:], count[0].astype(F32), F32)

    barrier = pltpu.get_barrier_semaphore()
    peers = [{n: shifted(n, d, 4)} for n in ("x", "y") for d in (1, 2, 3)] + [other_z, other_zh, other_core]
    for peer in peers:
        pl.semaphore_signal(barrier, inc=1, device_id=peer, device_id_type=MESH)
    pl.semaphore_wait(barrier, len(peers))

    def send_first(h, k):
        for l in range(2):
            for d in (2, 1, 3):
                dst = got1.at[l, d - 1, k, :, rows_of(h)]
                send(block_of(h, l, k, d), dst, (s1, q1), (h, l, d - 1, k), to_first(l, d))

    for l in range(2):
        for d in (1, 2, 3):
            i = l * 3 + d - 1
            send(weight.at[0], weight1.at[i], (ws, wq), i, to_first(l, d))
    waiting = [(h, k) for h in range(len(SPLITS)) for k in ORDER]
    for h, k in waiting[:AHEAD]:
        send_first(h, k)
    del waiting[:AHEAD]

    def row_loop(start, size, body):
        step = GROUP if size % GROUP == 0 else 16 if size % 16 == 0 else 8

        def one(i, carry):
            body(pl.ds(pl.multiple_of(start + i * step, 8), step))
            return carry

        lax.fori_loop(0, size // step, one, 0)

    def sum_first(h, l, k, which, dst):
        w = [weight[0, 0:1, :]] + [weight1[l * 3 + d, 0:1, :] for d in range(3)]

        def body(r):
            t = own[l, k, which, r, :].astype(F32) * w[0]
            for d in range(3):
                t = t + got1[l, d, k, which, r, :].astype(F32) * w[d + 1]
            dst[l, k, r, :] = t

        row_loop(STARTS[h], SPLITS[h], body)

    def once(key):
        fresh = key not in ready
        ready.add(key)
        return fresh

    def on_first(h, l, k):
        if once("weight1"):
            for i in range(6):
                arrived(weight1.at[i], (ws, wq), i, to_first(i // 3, i % 3 + 1))
            weight[1] = weight[0] + weight1[0] + weight1[1] + weight1[2]
        own_copies[h, l, k].wait()
        for d in range(3):
            arrived(got1.at[l, d, k, :, rows_of(h)], (s1, q1), (h, l, d, k), to_first(l, d + 1))
        sum_first(h, l, k, 1 - z, sent2)
        if once("sent1"):
            send(weight.at[1], weight2, (ws, wq), 6, other_z)
        sum_first(h, l, k, z, total)
        send(sent2.at[l, k, rows_of(h)], got2.at[l, k, rows_of(h)], (s2, q2), (h, l, k), other_z)
        if not once((h, k)) and waiting:
            send_first(*waiting.pop(0))

    def give(h, l, k):
        if not once(("give", h, l, k)):
            r = rows_of(h)
            send(total.at[l, k, r], got3.at[l, k // 2, r], (s3, q3), (h, l, k // 2), to_last(l, k))

    def on_second(h, l, k):
        if once("weight2"):
            arrived(weight2, (ws, wq), 6, other_z)
            weight[2] = weight[1] + weight2[...]
        elif once("sent2"):
            for d in (1, 2, 3):
                send(weight.at[2], weight3.at[d - 1], (ws, wq), 6 + d, to_last(0, d))
        arrived(got2.at[l, k, rows_of(h)], (s2, q2), (h, l, k), other_z)

        def body(r):
            total[l, k, r, :] = total[l, k, r, :] + got2[l, k, r, :]

        row_loop(STARTS[h], SPLITS[h], body)
        if k == 2:
            for way in (1, 3):
                r = half_of(h, way)
                send(total.at[l, 2, r], gotm.at[l, r], (sm, qm), (h, l, way // 2), to_last(l, way))
        elif k:
            give(h, l, k)

    def on_merge(h, l, way):
        part_rows = half_of(h, way)
        arrived(gotm.at[l, part_rows], (sm, qm), (h, l, way // 2), to_last(l, way))

        def body(r):
            total[l, way, r, :] = total[l, way, r, :] + gotm[l, r, :]

        row_loop(part_rows.start, part_rows.size, body)
        give(h, l, way)

    inv_one = 1.0 / (1.0 - 0.9**STEP)
    inv_two = 1.0 / (1.0 - 0.999**STEP)

    def on_final(h, l):
        if once("weight3"):
            for copy in state:
                copy.wait()
            for d in range(3):
                arrived(weight3.at[d], (ws, wq), 7 + d, to_last(0, d + 1))
            weight[3] = 1.0 / (weight[2] + weight3[0] + weight3[1] + weight3[2])
        scale = weight[3, 0:1, :]
        for i in range(2):
            arrived(got3.at[l, i, rows_of(h)], (s3, q3), (h, l, i), to_last(l, 1 + 2 * i))

        def body(r):
            grad = (total[l, 0, r, :] + got3[l, 0, r, :] + got3[l, 1, r, :]) * scale
            first = 0.9 * mom1_v[l, r, :] + 0.1 * grad
            second = 0.999 * mom2_v[l, r, :] + 0.001 * grad * grad
            direction = (first * inv_one) / (jnp.sqrt(second * inv_two) + 1e-08)
            old = par_v[l, r, :]
            new_par[l, r, :] = old - 0.001 * (direction + 0.1 * old)
            new_mom1[l, r, :] = first
            new_mom2[l, r, :] = second
            cands[h * 2 + l][me_tp, r, :] = direction.astype(BF16)

        row_loop(STARTS[h], SPLITS[h], body)
        mine = cands[h * 2 + l].at[me_tp, rows_of(h)]
        send(mine, mine, (ts, tq), (h, l, 0), other_zh)
        send(mine, mine, (ts, tq), (h, l, 1), other_core)

    tp_zh = (1 - at["zh"]) * 2 + at["core"]
    tp_core = at["zh"] * 2 + 1 - at["core"]
    tp_both = (1 - at["zh"]) * 2 + 1 - at["core"]

    def on_column(h, l):
        theirs = cands[h * 2 + l].at[tp_zh, rows_of(h)]
        arrived(theirs, (ts, tq), (h, l, 0), other_zh)
        send(theirs, theirs, (ts, tq), (h, l, 2), other_core)

    def block(h, l, ka, oz, kc):
        a = shifted(first_axis[l], 4 - ka, 4)
        c = shifted(last_axis[l], 4 - kc, 4)
        zz = 1 - z if oz else z
        return out.at[l, c, zz, a, rows_of(h)] if l == 0 else out.at[l, a, zz, c, rows_of(h)]

    def half_block(h, l, p, kc, way):
        a = shifted(first_axis[l], 4 - p % 4, 4)
        c = shifted(last_axis[l], 4 - kc, 4)
        zz = 1 - z if p // 4 else z
        r = half_of(h, way)
        return out.at[l, c, zz, a, r] if l == 0 else out.at[l, a, zz, c, r]

    def spread_last(h, l, p):
        b = block(h, l, p % 4, p // 4, 0)
        for way in (1, 3):
            send(b, b, (cs, cq), (h, l, way // 2, p), to_last(l, way))

    def spread_z(h, l, d):
        b = block(h, l, d, 0, 0)
        send(b, b, (zs, zq), (h, l, d), other_z)

    def on_pick(h, l):
        cand = cands[h * 2 + l]
        arrived(cand.at[tp_core, rows_of(h)], (ts, tq), (h, l, 1), other_core)
        arrived(cand.at[tp_both, rows_of(h)], (ts, tq), (h, l, 2), other_core)
        wanted = owners[l, me_tp]
        y, x = at["y"], at["x"]

        def body(r):
            out[l, y, z, x, r, :] = cand[wanted, r, :]

        row_loop(STARTS[h], SPLITS[h], body)
        mine = block(h, l, 0, 0, 0)
        for d in (1, 3, 2):
            send(mine, mine, (as_, aq), (h, l, d - 1), to_first(l, d))
        spread_z(h, l, 0)
        spread_last(h, l, 0)

    def on_near(h, l, d):
        arrived(block(h, l, d, 0, 0), (as_, aq), (h, l, d - 1), to_first(l, d))
        spread_last(h, l, d)
        spread_z(h, l, d)

    def on_z(h, l, d):
        arrived(block(h, l, d, 1, 0), (zs, zq), (h, l, d), other_z)
        spread_last(h, l, 4 + d)

    def on_ring(h, l, p, way):
        arrived(block(h, l, p % 4, p // 4, way), (cs, cq), (h, l, way // 2, p), to_last(l, way))
        piece = half_block(h, l, p, way, way)
        send(piece, piece, (hs, hq), (h, l, way // 2, p), to_last(l, way))

    handlers = {
        "s1": on_first, "s2": on_second, "m": on_merge, "fin": on_final, "tz": on_column,
        "ag": on_pick, "A": on_near, "Z": on_z, "C": on_ring,
    }
    for name, *args in EVENTS:
        handlers[name](*args)
    for name, *args in EVENTS:
        if name == "C":
            h, l, p, way = args
            arrived(half_block(h, l, p, 2, way), (hs, hq), (h, l, way // 2, p), to_last(l, way))
    for copy in pending:
        copy.wait_send()


def flush(a, b, c, d, oa, ob, oc, od, sems):
    copies = [
        pltpu.make_async_copy(src, dst, sems.at[i])
        for i, (src, dst) in enumerate(((d, od), (a, oa), (b, ob), (c, oc)))
    ]
    for copy in copies:
        copy.start()
    for copy in copies:
        copy.wait()


def local(partials, token_counts, owner_map, params, moment1, moment2):
    layers, shard, cols = params.shape
    blocks = partials.reshape(layers, 4, 2, 4, shard, cols)
    hbm = pl.BlockSpec(memory_space=pltpu.HBM)
    vmem = pl.BlockSpec(memory_space=pltpu.VMEM)
    dma = pltpu.SemaphoreType.DMA
    tile = (shard, cols)
    parts = len(SPLITS)
    results = pl.pallas_call(
        kernel,
        out_shape=(
            pltpu.VMEM(params.shape, F32),
            pltpu.VMEM(params.shape, F32),
            pltpu.VMEM(params.shape, F32),
            pltpu.VMEM((layers, 4, 2, 4, *tile), BF16),
        ),
        in_specs=[hbm] * 6,
        out_specs=(vmem, vmem, vmem, vmem),
        scratch_shapes=[
            pltpu.SMEM((1,), jnp.int32),
            pltpu.SMEM((2, 4), jnp.int32),
            pltpu.VMEM((2, 4, 2, *tile), BF16),
            pltpu.VMEM((2, 3, 4, 2, *tile), BF16),
            pltpu.VMEM((2, 4, *tile), F32),
            pltpu.VMEM((2, 4, *tile), F32),
            pltpu.VMEM((2, 4, *tile), F32),
            pltpu.VMEM((2, *tile), F32),
            pltpu.VMEM((2, 2, *tile), F32),
            pltpu.VMEM((4, 8, cols), F32),
            pltpu.VMEM((6, 8, cols), F32),
            pltpu.VMEM((8, cols), F32),
            pltpu.VMEM((3, 8, cols), F32),
            pltpu.VMEM(params.shape, F32),
            pltpu.VMEM(params.shape, F32),
            pltpu.VMEM(params.shape, F32),
            dma((5,)),
            dma((parts, 2, 4)),
            dma((parts, 2, 3, 4)), dma((parts, 2, 3, 4)),
            dma((parts, 2, 4)), dma((parts, 2, 4)),
            dma((parts, 2, 2)), dma((parts, 2, 2)),
            dma((parts, 2, 2)), dma((parts, 2, 2)),
            dma((10,)), dma((10,)),
            dma((parts, 2, 3)), dma((parts, 2, 3)),
            dma((parts, 2, 3)), dma((parts, 2, 3)),
            dma((parts, 2, 4)), dma((parts, 2, 4)),
            dma((parts, 2, 2, 8)), dma((parts, 2, 2, 8)),
            dma((parts, 2, 2, 8)), dma((parts, 2, 2, 8)),
            *[pltpu.VMEM((4, *tile), BF16) for _ in range(2 * parts)],
        ],
        compiler_params=pltpu.CompilerParams(
            collective_id=0, has_side_effects=True, vmem_limit_bytes=56 * 2**20
        ),
        name="reduce_update_spread",
    )(blocks, token_counts, owner_map, params, moment1, moment2)
    new_params, first, second, rollout = pl.pallas_call(
        flush,
        out_shape=tuple(jax.ShapeDtypeStruct(r.shape, r.dtype) for r in results),
        in_specs=[vmem] * 4,
        out_specs=(pl.BlockSpec(memory_space=pl.ANY),) * 4,
        scratch_shapes=[dma((4,))],
        compiler_params=pltpu.CompilerParams(vmem_limit_bytes=2**20),
        name="flush",
    )(*results)
    return new_params, first, second, rollout.reshape(layers, 32 * shard, cols)


def solution(mesh):
    split = Mesh(mesh.devices.reshape(4, 2, 4, 2, 2), AXES)
    return jax.shard_map(
        local,
        mesh=split,
        in_specs=(
            P(FSDP, None, None, TP),
            P(FSDP),
            P(),
            P(None, FSDP, TP),
            P(None, FSDP, TP),
            P(None, FSDP, TP),
        ),
        out_specs=(P(None, FSDP, TP), P(None, FSDP, TP), P(None, FSDP, TP), P(None, None, TP)),
        check_vma=False,
    )
```

```python
import jax
import jax.numpy as jnp
from jax import lax
from jax.experimental import pallas as pl
from jax.experimental.pallas import tpu as pltpu
from jax.sharding import Mesh
from jax.sharding import PartitionSpec as P

STEP = 10
AXES = ("y", "zl", "x", "zh", "core")
FSDP = ("y", "zl", "x")
TP = ("zh", "core")
MESH = pl.DeviceIdType.MESH
F32 = jnp.float32
BF16 = jnp.bfloat16
GROUP = 32
ORDER = (2, 1, 3, 0)
SPLITS = (96, 64)
STARTS = tuple(sum(SPLITS[:i]) for i in range(len(SPLITS)))
AHEAD = 2
EVENTS = [
    ("s1", 0, 0, 2), ("s1", 0, 1, 2), ("s1", 0, 0, 1), ("s1", 0, 1, 1), ("s2", 0, 0, 2), ("s2", 0, 1, 2),
    ("s1", 0, 0, 3), ("s1", 0, 1, 3), ("s2", 0, 0, 1), ("s2", 0, 1, 1), ("s1", 0, 0, 0), ("s1", 0, 1, 0),
    ("s2", 0, 0, 3), ("m", 0, 0, 1), ("m", 0, 0, 3), ("m", 0, 1, 1), ("m", 0, 1, 3), ("s2", 0, 1, 3),
    ("s1", 1, 0, 2), ("s1", 1, 1, 2), ("s2", 0, 0, 0), ("s1", 1, 0, 1), ("s1", 1, 1, 1), ("s2", 0, 1, 0),
    ("s2", 1, 0, 2), ("fin", 0, 0), ("fin", 0, 1), ("s2", 1, 1, 2), ("s2", 1, 0, 1), ("s1", 1, 0, 3),
    ("s1", 1, 1, 3), ("s2", 1, 1, 1), ("tz", 0, 0), ("tz", 0, 1), ("ag", 0, 0), ("s1", 1, 0, 0), ("s1", 1, 1, 0),
    ("ag", 0, 1), ("m", 1, 0, 1), ("m", 1, 0, 3), ("m", 1, 1, 1), ("m", 1, 1, 3), ("s2", 1, 0, 3), ("s2", 1, 1, 3),
    ("A", 0, 0, 1), ("C", 0, 0, 0), ("Z", 0, 0, 0), ("A", 0, 1, 1), ("A", 0, 0, 2), ("C", 0, 1, 0),
    ("s2", 1, 0, 0), ("A", 0, 1, 2), ("s2", 1, 1, 0), ("fin", 1, 1), ("fin", 1, 0), ("C", 0, 1, 1), ("Z", 0, 1, 0),
    ("C", 0, 0, 1), ("C", 0, 1, 3), ("Z", 0, 0, 1), ("C", 0, 0, 3), ("Z", 0, 0, 3), ("C", 0, 1, 2), ("tz", 1, 1),
    ("C", 0, 0, 4), ("Z", 0, 1, 1), ("tz", 1, 0), ("ag", 1, 1), ("C", 0, 0, 2), ("C", 0, 1, 4), ("Z", 0, 1, 3),
    ("ag", 1, 0), ("Z", 0, 0, 2), ("C", 0, 0, 5), ("C", 0, 1, 5), ("Z", 0, 1, 2), ("C", 0, 0, 7), ("C", 1, 1, 0),
    ("Z", 1, 1, 0), ("A", 1, 1, 1), ("Z", 1, 0, 0), ("C", 0, 1, 7), ("A", 1, 0, 1), ("A", 1, 1, 2), ("C", 1, 0, 0),
    ("A", 1, 0, 2), ("Z", 1, 1, 1), ("C", 0, 0, 6), ("Z", 1, 1, 3), ("C", 0, 1, 6), ("Z", 1, 0, 1), ("C", 1, 1, 4),
    ("Z", 1, 0, 3), ("C", 1, 0, 4), ("C", 1, 1, 1), ("Z", 1, 1, 2), ("C", 1, 0, 1), ("C", 1, 1, 3), ("Z", 1, 0, 2),
    ("C", 1, 0, 3), ("C", 1, 1, 2), ("C", 1, 0, 2), ("C", 1, 1, 5), ("C", 1, 0, 5), ("C", 1, 1, 7), ("C", 1, 0, 7),
    ("C", 1, 1, 6), ("C", 1, 0, 6),
]


def kernel(
    part, count_h, owners_h, par, mom1, mom2,
    new_par, new_mom1, new_mom2, out,
    count, owners, own, got1, sent2, total, got2, gotm, got3,
    weight, weight1, weight2, weight3, state,
    local_sem, own_sem, sent, q1, q2, qm, q3, wq, tq, aq, zq, cq, hq,
    *cands,
):
    at = {name: lax.axis_index(name) for name in AXES}
    z = at["zl"]
    me_tp = at["zh"] * 2 + at["core"]
    first_axis = ("x", "y")
    last_axis = ("y", "x")
    ready = set()

    def rows_of(h):
        return pl.ds(STARTS[h], SPLITS[h])

    def half_of(h, way):
        n = SPLITS[h] // 2
        return pl.ds(STARTS[h] + (n if way == 3 else 0), n)

    def shifted(name, by, size):
        return lax.rem(at[name] + by, size)

    def to_first(l, d):
        return {first_axis[l]: shifted(first_axis[l], d, 4)}

    def to_last(l, d):
        return {last_axis[l]: shifted(last_axis[l], d, 4)}

    other_z = {"zl": 1 - z}
    other_zh = {"zh": 1 - at["zh"]}
    other_core = {"core": 1 - at["core"]}

    def send(src, dst, kind, sem, device):
        pltpu.make_async_remote_copy(
            src_ref=src, dst_ref=dst, send_sem=sent.at[kind], recv_sem=sem, device_id=device, device_id_type=MESH
        ).start()

    def arrived(ref, sem):
        pltpu.make_async_copy(ref, ref, sem).wait()

    def block_of(h, l, k, to):
        c = shifted(last_axis[l], k, 4)
        a = shifted(first_axis[l], to, 4)
        return part.at[0, c, :, a, rows_of(h)] if l == 0 else part.at[1, a, :, c, rows_of(h)]

    scalars = [
        pltpu.make_async_copy(count_h, count, local_sem.at[0]),
        pltpu.make_async_copy(owners_h, owners, local_sem.at[1]),
    ]
    for copy in scalars:
        copy.start()
    for h in range(len(SPLITS)):
        for k in ORDER:
            for l in range(2):
                pltpu.make_async_copy(block_of(h, l, k, 0), own.at[l, k, :, rows_of(h)], own_sem.at[h]).start()
    for i, source in enumerate((par, mom1, mom2)):
        pltpu.make_async_copy(source, state.at[i], local_sem.at[2]).start()
    for copy in scalars:
        copy.wait()
    weight[0] = jnp.full(weight.shape[1:], count[0].astype(F32), F32)

    barrier = pltpu.get_barrier_semaphore()
    peers = [{n: shifted(n, d, 4)} for n in ("x", "y") for d in (1, 2, 3)] + [other_z, other_zh, other_core]
    for peer in peers:
        pl.semaphore_signal(barrier, inc=1, device_id=peer, device_id_type=MESH)
    pl.semaphore_wait(barrier, len(peers))

    def send_first(h, k):
        for l in range(2):
            for d in (2, 1, 3):
                dst = got1.at[l, d - 1, k, :, rows_of(h)]
                send(block_of(h, l, k, d), dst, 0, q1.at[h, l, k], to_first(l, d))

    for l in range(2):
        for d in (1, 2, 3):
            i = l * 3 + d - 1
            send(weight.at[0], weight1.at[i], 4, wq.at[0], to_first(l, d))
    waiting = [(h, k) for h in range(len(SPLITS)) for k in ORDER]
    for h, k in waiting[:AHEAD]:
        send_first(h, k)
    del waiting[:AHEAD]

    def row_loop(start, size, body):
        step = GROUP if size % GROUP == 0 else 16 if size % 16 == 0 else 8

        def one(i, carry):
            body(pl.ds(pl.multiple_of(start + i * step, 8), step))
            return carry

        lax.fori_loop(0, size // step, one, 0)

    def sum_first(h, l, k, which, dst):
        w = [weight[0, 0:1, :]] + [weight1[l * 3 + d, 0:1, :] for d in range(3)]

        def body(r):
            t = own[l, k, which, r, :].astype(F32) * w[0]
            for d in range(3):
                t = t + got1[l, d, k, which, r, :].astype(F32) * w[d + 1]
            dst[l, k, r, :] = t

        row_loop(STARTS[h], SPLITS[h], body)

    def once(key):
        fresh = key not in ready
        ready.add(key)
        return fresh

    def on_first(h, l, k):
        if once("weight1"):
            arrived(weight1, wq.at[0])
            weight[1] = weight[0] + weight1[0] + weight1[1] + weight1[2]
        if once(("own", h)):
            arrived(own.at[:, :, :, rows_of(h)], own_sem.at[h])
        arrived(got1.at[l, :, k, :, rows_of(h)], q1.at[h, l, k])
        sum_first(h, l, k, 1 - z, sent2)
        if once("sent1"):
            send(weight.at[1], weight2, 5, wq.at[1], other_z)
        sum_first(h, l, k, z, total)
        send(sent2.at[l, k, rows_of(h)], got2.at[l, k, rows_of(h)], 1, q2.at[h, l, k], other_z)
        if not once((h, k)) and waiting:
            send_first(*waiting.pop(0))

    def give(h, l, k):
        if not once(("give", h, l, k)):
            r = rows_of(h)
            send(total.at[l, k, r], got3.at[l, k // 2, r], 3, q3.at[h, l], to_last(l, k))

    def on_second(h, l, k):
        if once("weight2"):
            arrived(weight2, wq.at[1])
            weight[2] = weight[1] + weight2[...]
        elif once("sent2"):
            for d in (1, 2, 3):
                send(weight.at[2], weight3.at[d - 1], 6, wq.at[2], to_last(0, d))
        arrived(got2.at[l, k, rows_of(h)], q2.at[h, l, k])

        def body(r):
            total[l, k, r, :] = total[l, k, r, :] + got2[l, k, r, :]

        row_loop(STARTS[h], SPLITS[h], body)
        if k == 2:
            for way in (1, 3):
                r = half_of(h, way)
                send(total.at[l, 2, r], gotm.at[l, r], 2, qm.at[h, l, way // 2], to_last(l, way))
        elif k:
            give(h, l, k)

    def on_merge(h, l, way):
        part_rows = half_of(h, way)
        arrived(gotm.at[l, part_rows], qm.at[h, l, way // 2])

        def body(r):
            total[l, way, r, :] = total[l, way, r, :] + gotm[l, r, :]

        row_loop(part_rows.start, part_rows.size, body)
        give(h, l, way)

    inv_one = 1.0 / (1.0 - 0.9**STEP)
    inv_two = 1.0 / (1.0 - 0.999**STEP)

    def on_final(h, l):
        if once("weight3"):
            arrived(state, local_sem.at[2])
            arrived(weight3, wq.at[2])
            weight[3] = 1.0 / (weight[2] + weight3[0] + weight3[1] + weight3[2])
        scale = weight[3, 0:1, :]
        arrived(got3.at[l, :, rows_of(h)], q3.at[h, l])

        def body(r):
            grad = (total[l, 0, r, :] + got3[l, 0, r, :] + got3[l, 1, r, :]) * scale
            first = 0.9 * state[1, l, r, :] + 0.1 * grad
            second = 0.999 * state[2, l, r, :] + 0.001 * grad * grad
            direction = (first * inv_one) / (jnp.sqrt(second * inv_two) + 1e-08)
            old = state[0, l, r, :]
            new_par[l, r, :] = old - 0.001 * (direction + 0.1 * old)
            new_mom1[l, r, :] = first
            new_mom2[l, r, :] = second
            cands[h * 2 + l][me_tp, r, :] = direction.astype(BF16)

        row_loop(STARTS[h], SPLITS[h], body)
        mine = cands[h * 2 + l].at[me_tp, rows_of(h)]
        send(mine, mine, 7, tq.at[h, l, 0], other_zh)
        send(mine, mine, 7, tq.at[h, l, 1], other_core)

    tp_zh = (1 - at["zh"]) * 2 + at["core"]
    tp_core = at["zh"] * 2 + 1 - at["core"]
    tp_both = (1 - at["zh"]) * 2 + 1 - at["core"]

    def on_column(h, l):
        theirs = cands[h * 2 + l].at[tp_zh, rows_of(h)]
        arrived(theirs, tq.at[h, l, 0])
        send(theirs, theirs, 7, tq.at[h, l, 1], other_core)

    def block(h, l, ka, oz, kc):
        a = shifted(first_axis[l], 4 - ka, 4)
        c = shifted(last_axis[l], 4 - kc, 4)
        zz = 1 - z if oz else z
        return out.at[l, c, zz, a, rows_of(h)] if l == 0 else out.at[l, a, zz, c, rows_of(h)]

    def half_block(h, l, p, kc, way):
        a = shifted(first_axis[l], 4 - p % 4, 4)
        c = shifted(last_axis[l], 4 - kc, 4)
        zz = 1 - z if p // 4 else z
        r = half_of(h, way)
        return out.at[l, c, zz, a, r] if l == 0 else out.at[l, a, zz, c, r]

    def spread_last(h, l, p):
        b = block(h, l, p % 4, p // 4, 0)
        for way in (1, 3):
            send(b, b, 8, cq.at[h, l, p], to_last(l, way))

    def spread_z(h, l, d):
        b = block(h, l, d, 0, 0)
        send(b, b, 9, zq.at[h, l, d], other_z)

    def on_pick(h, l):
        cand = cands[h * 2 + l]
        arrived(cand.at[pl.ds(0, 2), rows_of(h)], tq.at[h, l, 1])
        wanted = owners[l, me_tp]
        y, x = at["y"], at["x"]

        def body(r):
            out[l, y, z, x, r, :] = cand[wanted, r, :]

        row_loop(STARTS[h], SPLITS[h], body)
        mine = block(h, l, 0, 0, 0)
        for d in (1, 3, 2):
            send(mine, mine, 7, aq.at[h, l, d // 2 if d == 2 else 0], to_first(l, d))
        spread_z(h, l, 0)
        spread_last(h, l, 0)

    def on_near(h, l, d):
        if d == 2:
            arrived(block(h, l, 2, 0, 0), aq.at[h, l, 1])
        else:
            arrived(out.at[0, pl.ds(0, 2), 0, 0, rows_of(h)], aq.at[h, l, 0])
        for i in (2,) if d == 2 else (1, 3):
            spread_last(h, l, i)
            spread_z(h, l, i)

    def on_z(h, l, d):
        arrived(block(h, l, d, 1, 0), zq.at[h, l, d])
        spread_last(h, l, 4 + d)

    def on_ring(h, l, p):
        arrived(out.at[0, pl.ds(0, 2), 0, 0, rows_of(h)], cq.at[h, l, p])
        for way in (1, 3):
            piece = half_block(h, l, p, way, way)
            send(piece, piece, 10, hq.at[0], to_last(l, way))

    handlers = {
        "s1": on_first, "s2": on_second, "m": on_merge, "fin": on_final, "tz": on_column,
        "ag": on_pick, "A": on_near, "Z": on_z, "C": on_ring,
    }
    for name, *args in EVENTS:
        handlers[name](*args)
    arrived(out.at[0, pl.ds(0, 2)], hq.at[0])
    for i, ref in enumerate((
        got1, sent2, gotm, got3, weight1, weight2, weight3,
        out.at[0, pl.ds(0, 3), 0], out.at[0], out.at[0, 0], out.at[0, pl.ds(0, 2)],
    )):
        arrived(ref, sent.at[i])


def flush(a, b, c, d, oa, ob, oc, od, sems):
    copies = [
        pltpu.make_async_copy(src, dst, sems.at[i])
        for i, (src, dst) in enumerate(((d, od), (a, oa), (b, ob), (c, oc)))
    ]
    for copy in copies:
        copy.start()
    for copy in copies:
        copy.wait()


def local(partials, token_counts, owner_map, params, moment1, moment2):
    layers, shard, cols = params.shape
    blocks = partials.reshape(layers, 4, 2, 4, shard, cols)
    hbm = pl.BlockSpec(memory_space=pltpu.HBM)
    vmem = pl.BlockSpec(memory_space=pltpu.VMEM)
    dma = pltpu.SemaphoreType.DMA
    tile = (shard, cols)
    parts = len(SPLITS)
    results = pl.pallas_call(
        kernel,
        out_shape=(
            pltpu.VMEM(params.shape, F32),
            pltpu.VMEM(params.shape, F32),
            pltpu.VMEM(params.shape, F32),
            pltpu.VMEM((layers, 4, 2, 4, *tile), BF16),
        ),
        in_specs=[hbm] * 6,
        out_specs=(vmem, vmem, vmem, vmem),
        scratch_shapes=[
            pltpu.SMEM((1,), jnp.int32),
            pltpu.SMEM((2, 4), jnp.int32),
            pltpu.VMEM((2, 4, 2, *tile), BF16),
            pltpu.VMEM((2, 3, 4, 2, *tile), BF16),
            pltpu.VMEM((2, 4, *tile), F32),
            pltpu.VMEM((2, 4, *tile), F32),
            pltpu.VMEM((2, 4, *tile), F32),
            pltpu.VMEM((2, *tile), F32),
            pltpu.VMEM((2, 2, *tile), F32),
            pltpu.VMEM((4, 8, cols), F32),
            pltpu.VMEM((6, 8, cols), F32),
            pltpu.VMEM((8, cols), F32),
            pltpu.VMEM((3, 8, cols), F32),
            pltpu.VMEM((3, *params.shape), F32),
            dma((3,)),
            dma((parts,)),
            dma((11,)),
            dma((parts, 2, 4)),
            dma((parts, 2, 4)),
            dma((parts, 2, 2)),
            dma((parts, 2)),
            dma((3,)),
            dma((parts, 2, 2)),
            dma((parts, 2, 2)),
            dma((parts, 2, 4)),
            dma((parts, 2, 8)),
            dma((1,)),
            *[pltpu.VMEM((4, *tile), BF16) for _ in range(2 * parts)],
        ],
        compiler_params=pltpu.CompilerParams(
            collective_id=0, has_side_effects=True, vmem_limit_bytes=56 * 2**20
        ),
        name="reduce_update_spread",
    )(blocks, token_counts, owner_map, params, moment1, moment2)
    new_params, first, second, rollout = pl.pallas_call(
        flush,
        out_shape=tuple(jax.ShapeDtypeStruct(r.shape, r.dtype) for r in results),
        in_specs=[vmem] * 4,
        out_specs=(pl.BlockSpec(memory_space=pl.ANY),) * 4,
        scratch_shapes=[dma((4,))],
        compiler_params=pltpu.CompilerParams(vmem_limit_bytes=2**20),
        name="flush",
    )(*results)
    return new_params, first, second, rollout.reshape(layers, 32 * shard, cols)


def solution(mesh):
    split = Mesh(mesh.devices.reshape(4, 2, 4, 2, 2), AXES)
    return jax.shard_map(
        local,
        mesh=split,
        in_specs=(
            P(FSDP, None, None, TP),
            P(FSDP),
            P(),
            P(None, FSDP, TP),
            P(None, FSDP, TP),
            P(None, FSDP, TP),
        ),
        out_specs=(P(None, FSDP, TP), P(None, FSDP, TP), P(None, FSDP, TP), P(None, None, TP)),
        check_vma=False,
    )
```

```python
import jax
import jax.numpy as jnp
from jax import lax
from jax.experimental import pallas as pl
from jax.experimental.pallas import tpu as pltpu
from jax.sharding import Mesh
from jax.sharding import PartitionSpec as P

STEP = 10
AXES = ("y", "zl", "x", "zh", "core")
FSDP = ("y", "zl", "x")
TP = ("zh", "core")
MESH = pl.DeviceIdType.MESH
F32 = jnp.float32
BF16 = jnp.bfloat16
GROUP = 32
ORDER = (2, 1, 3, 0)
SPLITS = (64, 48, 48)
STARTS = tuple(sum(SPLITS[:i]) for i in range(len(SPLITS)))
AHEAD = 3
EVENTS = [
    ("s1", 0, 0, 2), ("s1", 0, 1, 2), ("s1", 0, 0, 1), ("s1", 0, 1, 1), ("s2", 0, 0, 2), ("s2", 0, 1, 2),
    ("s1", 0, 0, 3), ("s1", 0, 1, 3), ("s2", 0, 0, 1), ("s2", 0, 1, 1), ("s1", 0, 0, 0), ("s1", 0, 1, 0),
    ("s2", 0, 0, 3), ("s1", 1, 0, 2), ("s1", 1, 1, 2), ("s2", 0, 1, 3), ("m", 0, 0, 1), ("m", 0, 0, 3),
    ("m", 0, 1, 1), ("m", 0, 1, 3), ("s2", 0, 0, 0), ("s1", 1, 0, 1), ("s1", 1, 1, 1), ("s2", 0, 1, 0),
    ("s2", 1, 0, 2), ("s1", 1, 0, 3), ("s1", 1, 1, 3), ("s2", 1, 1, 2), ("s2", 1, 0, 1), ("s1", 1, 0, 0),
    ("s1", 1, 1, 0), ("s2", 1, 1, 1), ("fin", 0, 0), ("fin", 0, 1), ("s2", 1, 0, 3), ("s2", 1, 1, 3),
    ("s1", 2, 0, 2), ("s1", 2, 1, 2), ("s2", 1, 0, 0), ("m", 1, 0, 1), ("m", 1, 0, 3), ("s2", 1, 1, 0),
    ("s1", 2, 0, 1), ("s1", 2, 1, 1), ("m", 1, 1, 1), ("m", 1, 1, 3), ("tz", 0, 0), ("tz", 0, 1), ("s2", 2, 0, 2),
    ("ag", 0, 0), ("ag", 0, 1), ("s1", 2, 0, 3), ("s1", 2, 1, 3), ("s2", 2, 1, 2), ("s2", 2, 0, 1),
    ("s1", 2, 0, 0), ("s1", 2, 1, 0), ("s2", 2, 1, 1), ("Z", 0, 0, 0), ("fin", 1, 0), ("fin", 1, 1),
    ("Z", 0, 1, 0), ("m", 2, 0, 1), ("m", 2, 0, 3), ("A", 0, 0, 1), ("C", 0, 0, 0), ("s2", 2, 0, 3),
    ("A", 0, 1, 1), ("C", 0, 1, 0), ("A", 0, 0, 2), ("s2", 2, 1, 3), ("m", 2, 1, 1), ("m", 2, 1, 3),
    ("C", 0, 0, 4), ("A", 0, 1, 2), ("s2", 2, 0, 0), ("C", 0, 1, 4), ("s2", 2, 1, 0), ("C", 0, 0, 1),
    ("C", 0, 1, 1), ("C", 0, 0, 3), ("C", 0, 1, 3), ("tz", 1, 0), ("fin", 2, 0), ("Z", 0, 0, 1), ("tz", 1, 1),
    ("C", 0, 0, 2), ("Z", 0, 0, 3), ("ag", 1, 0), ("fin", 2, 1), ("ag", 1, 1), ("Z", 0, 1, 1), ("C", 0, 1, 2),
    ("Z", 0, 1, 3), ("Z", 0, 0, 2), ("C", 0, 0, 5), ("Z", 0, 1, 2), ("A", 1, 0, 1), ("C", 0, 0, 7), ("Z", 1, 0, 0),
    ("C", 1, 0, 0), ("tz", 2, 0), ("C", 1, 1, 0), ("A", 1, 0, 2), ("A", 1, 1, 1), ("C", 0, 1, 5), ("Z", 1, 1, 0),
    ("tz", 2, 1), ("ag", 2, 0), ("C", 0, 0, 6), ("A", 1, 1, 2), ("C", 0, 1, 7), ("Z", 1, 0, 1), ("ag", 2, 1),
    ("C", 0, 1, 6), ("Z", 1, 0, 3), ("C", 1, 0, 1), ("C", 1, 0, 3), ("Z", 1, 0, 2), ("C", 1, 1, 1), ("Z", 1, 1, 1),
    ("C", 1, 0, 4), ("C", 1, 1, 3), ("Z", 1, 1, 3), ("C", 1, 0, 2), ("Z", 2, 0, 0), ("C", 1, 1, 4), ("C", 2, 0, 0),
    ("Z", 1, 1, 2), ("A", 2, 0, 1), ("Z", 2, 1, 0), ("C", 1, 0, 5), ("C", 1, 1, 2), ("A", 2, 0, 2), ("A", 2, 1, 1),
    ("C", 2, 1, 0), ("C", 1, 0, 7), ("A", 2, 1, 2), ("Z", 2, 0, 1), ("C", 1, 1, 5), ("C", 1, 0, 6), ("Z", 2, 0, 3),
    ("C", 1, 1, 7), ("Z", 2, 0, 2), ("C", 2, 0, 4), ("C", 1, 1, 6), ("Z", 2, 1, 1), ("C", 2, 1, 4), ("C", 2, 0, 1),
    ("Z", 2, 1, 3), ("C", 2, 0, 3), ("Z", 2, 1, 2), ("C", 2, 1, 1), ("C", 2, 1, 3), ("C", 2, 0, 2), ("C", 2, 1, 2),
    ("C", 2, 0, 5), ("C", 2, 0, 7), ("C", 2, 1, 5), ("C", 2, 0, 6), ("C", 2, 1, 7), ("C", 2, 1, 6),
]


def kernel(
    part, count_h, owners_h, par, mom1, mom2,
    new_par, new_mom1, new_mom2, out,
    count, owners, own, got1, sent2, total, got2, gotm, got3,
    weight, weight1, weight2, weight3, state,
    local_sem, own_sem, sent, q1, q2, qm, q3, wq, tq, aq, zq, cq, hq,
    *cands,
):
    at = {name: lax.axis_index(name) for name in AXES}
    z = at["zl"]
    me_tp = at["zh"] * 2 + at["core"]
    first_axis = ("x", "y")
    last_axis = ("y", "x")
    ready = set()

    def rows_of(h):
        return pl.ds(STARTS[h], SPLITS[h])

    def half_of(h, way):
        n = SPLITS[h] // 2
        return pl.ds(STARTS[h] + (n if way == 3 else 0), n)

    def shifted(name, by, size):
        return lax.rem(at[name] + by, size)

    def to_first(l, d):
        return {first_axis[l]: shifted(first_axis[l], d, 4)}

    def to_last(l, d):
        return {last_axis[l]: shifted(last_axis[l], d, 4)}

    other_z = {"zl": 1 - z}
    other_zh = {"zh": 1 - at["zh"]}
    other_core = {"core": 1 - at["core"]}

    def send(src, dst, kind, sem, device):
        pltpu.make_async_remote_copy(
            src_ref=src, dst_ref=dst, send_sem=sent.at[kind], recv_sem=sem, device_id=device, device_id_type=MESH
        ).start()

    def arrived(ref, sem):
        pltpu.make_async_copy(ref, ref, sem).wait()

    def block_of(h, l, k, to):
        c = shifted(last_axis[l], k, 4)
        a = shifted(first_axis[l], to, 4)
        return part.at[0, c, :, a, rows_of(h)] if l == 0 else part.at[1, a, :, c, rows_of(h)]

    scalars = [
        pltpu.make_async_copy(count_h, count, local_sem.at[0]),
        pltpu.make_async_copy(owners_h, owners, local_sem.at[1]),
    ]
    barrier = pltpu.get_barrier_semaphore()
    peers = [{n: shifted(n, d, 4)} for n in ("x", "y") for d in (1, 2, 3)] + [other_z, other_zh, other_core]
    for peer in peers:
        pl.semaphore_signal(barrier, inc=1, device_id=peer, device_id_type=MESH)
    for copy in scalars:
        copy.start()
    for h in range(len(SPLITS)):
        for k in ORDER:
            for l in range(2):
                pltpu.make_async_copy(block_of(h, l, k, 0), own.at[l, k, :, rows_of(h)], own_sem.at[h]).start()
    for i, source in enumerate((par, mom1, mom2)):
        pltpu.make_async_copy(source, state.at[i], local_sem.at[2]).start()
    for copy in scalars:
        copy.wait()
    weight[0] = jnp.full(weight.shape[1:], count[0].astype(F32), F32)

    pl.semaphore_wait(barrier, len(peers))

    def send_first(h, k):
        for l in range(2):
            for d in (2, 1, 3):
                dst = got1.at[l, d - 1, k, :, rows_of(h)]
                send(block_of(h, l, k, d), dst, 0, q1.at[h, l, k], to_first(l, d))

    for l in range(2):
        for d in (1, 2, 3):
            i = l * 3 + d - 1
            send(weight.at[0], weight1.at[i], 4, wq.at[0], to_first(l, d))
    waiting = [(h, k) for h in range(len(SPLITS)) for k in ORDER]
    for h, k in waiting[:AHEAD]:
        send_first(h, k)
    del waiting[:AHEAD]

    def row_loop(start, size, body):
        step = GROUP if size % GROUP == 0 else 16 if size % 16 == 0 else 8

        def one(i, carry):
            body(pl.ds(pl.multiple_of(start + i * step, 8), step))
            return carry

        lax.fori_loop(0, size // step, one, 0)

    def sum_first(h, l, k, which, dst):
        w = [weight[0, 0:1, :]] + [weight1[l * 3 + d, 0:1, :] for d in range(3)]

        def body(r):
            t = own[l, k, which, r, :].astype(F32) * w[0]
            for d in range(3):
                t = t + got1[l, d, k, which, r, :].astype(F32) * w[d + 1]
            dst[l, k, r, :] = t

        row_loop(STARTS[h], SPLITS[h], body)

    def once(key):
        fresh = key not in ready
        ready.add(key)
        return fresh

    def on_first(h, l, k):
        if once("weight1"):
            arrived(weight1, wq.at[0])
            weight[1] = weight[0] + weight1[0] + weight1[1] + weight1[2]
        if once(("own", h)):
            arrived(own.at[:, :, :, rows_of(h)], own_sem.at[h])
        arrived(got1.at[l, :, k, :, rows_of(h)], q1.at[h, l, k])
        sum_first(h, l, k, 1 - z, sent2)
        if once("sent1"):
            send(weight.at[1], weight2, 5, wq.at[1], other_z)
        sum_first(h, l, k, z, total)
        send(sent2.at[l, k, rows_of(h)], got2.at[l, k, rows_of(h)], 1, q2.at[h, l, k], other_z)
        if not once((h, k)) and waiting:
            send_first(*waiting.pop(0))

    def give(h, l, k):
        if not once(("give", h, l, k)):
            r = rows_of(h)
            send(total.at[l, k, r], got3.at[l, k // 2, r], 3, q3.at[h, l], to_last(l, k))

    def on_second(h, l, k):
        if once("weight2"):
            arrived(weight2, wq.at[1])
            weight[2] = weight[1] + weight2[...]
        elif once("sent2"):
            for d in (1, 2, 3):
                send(weight.at[2], weight3.at[d - 1], 6, wq.at[2], to_last(0, d))
        arrived(got2.at[l, k, rows_of(h)], q2.at[h, l, k])

        def body(r):
            total[l, k, r, :] = total[l, k, r, :] + got2[l, k, r, :]

        row_loop(STARTS[h], SPLITS[h], body)
        if k == 2:
            for way in (1, 3):
                r = half_of(h, way)
                send(total.at[l, 2, r], gotm.at[l, r], 2, qm.at[h, l, way // 2], to_last(l, way))
        elif k:
            give(h, l, k)

    def on_merge(h, l, way):
        part_rows = half_of(h, way)
        arrived(gotm.at[l, part_rows], qm.at[h, l, way // 2])

        def body(r):
            total[l, way, r, :] = total[l, way, r, :] + gotm[l, r, :]

        row_loop(part_rows.start, part_rows.size, body)
        give(h, l, way)

    inv_one = 1.0 / (1.0 - 0.9**STEP)
    inv_two = 1.0 / (1.0 - 0.999**STEP)

    def on_final(h, l):
        if once("weight3"):
            arrived(state, local_sem.at[2])
            arrived(weight3, wq.at[2])
            weight[3] = 1.0 / (weight[2] + weight3[0] + weight3[1] + weight3[2])
        scale = weight[3, 0:1, :]
        arrived(got3.at[l, :, rows_of(h)], q3.at[h, l])

        def body(r):
            grad = (total[l, 0, r, :] + got3[l, 0, r, :] + got3[l, 1, r, :]) * scale
            first = 0.9 * state[1, l, r, :] + 0.1 * grad
            second = 0.999 * state[2, l, r, :] + 0.001 * grad * grad
            direction = (first * inv_one) / (jnp.sqrt(second * inv_two) + 1e-08)
            old = state[0, l, r, :]
            new_par[l, r, :] = old - 0.001 * (direction + 0.1 * old)
            new_mom1[l, r, :] = first
            new_mom2[l, r, :] = second
            cands[h * 2 + l][me_tp, r, :] = direction.astype(BF16)

        row_loop(STARTS[h], SPLITS[h], body)
        mine = cands[h * 2 + l].at[me_tp, rows_of(h)]
        send(mine, mine, 7, tq.at[h, l, 0], other_zh)
        send(mine, mine, 7, tq.at[h, l, 1], other_core)

    tp_zh = (1 - at["zh"]) * 2 + at["core"]
    tp_core = at["zh"] * 2 + 1 - at["core"]
    tp_both = (1 - at["zh"]) * 2 + 1 - at["core"]

    def on_column(h, l):
        theirs = cands[h * 2 + l].at[tp_zh, rows_of(h)]
        arrived(theirs, tq.at[h, l, 0])
        send(theirs, theirs, 7, tq.at[h, l, 1], other_core)

    def block(h, l, ka, oz, kc):
        a = shifted(first_axis[l], 4 - ka, 4)
        c = shifted(last_axis[l], 4 - kc, 4)
        zz = 1 - z if oz else z
        return out.at[l, c, zz, a, rows_of(h)] if l == 0 else out.at[l, a, zz, c, rows_of(h)]

    def half_block(h, l, p, kc, way):
        a = shifted(first_axis[l], 4 - p % 4, 4)
        c = shifted(last_axis[l], 4 - kc, 4)
        zz = 1 - z if p // 4 else z
        r = half_of(h, way)
        return out.at[l, c, zz, a, r] if l == 0 else out.at[l, a, zz, c, r]

    def spread_last(h, l, p):
        b = block(h, l, p % 4, p // 4, 0)
        for way in (1, 3):
            send(b, b, 8, cq.at[h, l, p], to_last(l, way))

    def spread_z(h, l, d):
        b = block(h, l, d, 0, 0)
        send(b, b, 9, zq.at[h, l, d], other_z)

    def on_pick(h, l):
        cand = cands[h * 2 + l]
        arrived(cand.at[pl.ds(0, 2), rows_of(h)], tq.at[h, l, 1])
        wanted = owners[l, me_tp]
        y, x = at["y"], at["x"]

        def body(r):
            out[l, y, z, x, r, :] = cand[wanted, r, :]

        row_loop(STARTS[h], SPLITS[h], body)
        mine = block(h, l, 0, 0, 0)
        for d in (1, 3, 2):
            send(mine, mine, 7, aq.at[h, l, d // 2 if d == 2 else 0], to_first(l, d))
        spread_z(h, l, 0)
        spread_last(h, l, 0)

    def on_near(h, l, d):
        if d == 2:
            arrived(block(h, l, 2, 0, 0), aq.at[h, l, 1])
        else:
            arrived(out.at[0, pl.ds(0, 2), 0, 0, rows_of(h)], aq.at[h, l, 0])
        for i in (2,) if d == 2 else (1, 3):
            spread_last(h, l, i)
            spread_z(h, l, i)

    def on_z(h, l, d):
        arrived(block(h, l, d, 1, 0), zq.at[h, l, d])
        spread_last(h, l, 4 + d)

    def on_ring(h, l, p):
        arrived(out.at[0, pl.ds(0, 2), 0, 0, rows_of(h)], cq.at[h, l, p])
        for way in (1, 3):
            piece = half_block(h, l, p, way, way)
            send(piece, piece, 10, hq.at[0], to_last(l, way))

    handlers = {
        "s1": on_first, "s2": on_second, "m": on_merge, "fin": on_final, "tz": on_column,
        "ag": on_pick, "A": on_near, "Z": on_z, "C": on_ring,
    }
    for name, *args in EVENTS:
        handlers[name](*args)
    arrived(out.at[0, pl.ds(0, 2)], hq.at[0])
    for i, ref in enumerate((
        got1, sent2, gotm, got3, weight1, weight2, weight3,
        out.at[0, pl.ds(0, 3), 0], out.at[0], out.at[0, 0], out.at[0, pl.ds(0, 2)],
    )):
        arrived(ref, sent.at[i])


def flush(a, b, c, d, oa, ob, oc, od, sems):
    pieces = [(d.at[l, i], od.at[l, i]) for l in range(2) for i in range(4)] + [(a, oa), (b, ob), (c, oc)]
    copies = [pltpu.make_async_copy(src, dst, sems.at[i]) for i, (src, dst) in enumerate(pieces)]
    for copy in copies:
        copy.start()
    for copy in copies:
        copy.wait()


def local(partials, token_counts, owner_map, params, moment1, moment2):
    layers, shard, cols = params.shape
    blocks = partials.reshape(layers, 4, 2, 4, shard, cols)
    hbm = pl.BlockSpec(memory_space=pltpu.HBM)
    vmem = pl.BlockSpec(memory_space=pltpu.VMEM)
    dma = pltpu.SemaphoreType.DMA
    tile = (shard, cols)
    parts = len(SPLITS)
    results = pl.pallas_call(
        kernel,
        out_shape=(
            pltpu.VMEM(params.shape, F32),
            pltpu.VMEM(params.shape, F32),
            pltpu.VMEM(params.shape, F32),
            pltpu.VMEM((layers, 4, 2, 4, *tile), BF16),
        ),
        in_specs=[hbm] * 6,
        out_specs=(vmem, vmem, vmem, vmem),
        scratch_shapes=[
            pltpu.SMEM((1,), jnp.int32),
            pltpu.SMEM((2, 4), jnp.int32),
            pltpu.VMEM((2, 4, 2, *tile), BF16),
            pltpu.VMEM((2, 3, 4, 2, *tile), BF16),
            pltpu.VMEM((2, 4, *tile), F32),
            pltpu.VMEM((2, 4, *tile), F32),
            pltpu.VMEM((2, 4, *tile), F32),
            pltpu.VMEM((2, *tile), F32),
            pltpu.VMEM((2, 2, *tile), F32),
            pltpu.VMEM((4, 8, cols), F32),
            pltpu.VMEM((6, 8, cols), F32),
            pltpu.VMEM((8, cols), F32),
            pltpu.VMEM((3, 8, cols), F32),
            pltpu.VMEM((3, *params.shape), F32),
            dma((3,)),
            dma((parts,)),
            dma((11,)),
            dma((parts, 2, 4)),
            dma((parts, 2, 4)),
            dma((parts, 2, 2)),
            dma((parts, 2)),
            dma((3,)),
            dma((parts, 2, 2)),
            dma((parts, 2, 2)),
            dma((parts, 2, 4)),
            dma((parts, 2, 8)),
            dma((1,)),
            *[pltpu.VMEM((4, *tile), BF16) for _ in range(2 * parts)],
        ],
        compiler_params=pltpu.CompilerParams(
            collective_id=0, has_side_effects=True, vmem_limit_bytes=56 * 2**20
        ),
        name="reduce_update_spread",
    )(blocks, token_counts, owner_map, params, moment1, moment2)
    new_params, first, second, rollout = pl.pallas_call(
        flush,
        out_shape=tuple(jax.ShapeDtypeStruct(r.shape, r.dtype) for r in results),
        in_specs=[vmem] * 4,
        out_specs=(pl.BlockSpec(memory_space=pl.ANY),) * 4,
        scratch_shapes=[dma((11,))],
        compiler_params=pltpu.CompilerParams(vmem_limit_bytes=2**20),
        name="flush",
    )(*results)
    return new_params, first, second, rollout.reshape(layers, 32 * shard, cols)


def solution(mesh):
    split = Mesh(mesh.devices.reshape(4, 2, 4, 2, 2), AXES)
    return jax.shard_map(
        local,
        mesh=split,
        in_specs=(
            P(FSDP, None, None, TP),
            P(FSDP),
            P(),
            P(None, FSDP, TP),
            P(None, FSDP, TP),
            P(None, FSDP, TP),
        ),
        out_specs=(P(None, FSDP, TP), P(None, FSDP, TP), P(None, FSDP, TP), P(None, None, TP)),
        check_vma=False,
    )
```
